32 devices in a mesh: seq: 8 (over z, x), tp: 4 (over y, core).
Axes of the slice: x: 2, y: 2, z: 4, core: 2. Of those that a mesh axis runs over, the one named last changes fastest.
Arguments:
- queries: bfloat16 [2048, 8192], P('seq', 'tp'), may hold values from -120 to 120
- keys: bfloat16 [2048, 1024], P('seq', 'tp'), may hold values from -5 to 5
- values: bfloat16 [2048, 1024], P('seq', 'tp'), may hold values from -6 to 6
- w_query: bfloat16 [8192, 8192], P('seq', 'tp'), may hold values from -0.0625 to 0.0625
- key_weight: bfloat16 [8192, 1024], P('seq'), may hold values from -0.0625 to 0.0625
Outputs:
- attended: bfloat16 [2048, 8192], P('seq', 'tp')
- head_logit_maxima: float32 [64], P('tp')
- w_query_clipped: bfloat16 [8192, 8192], P('seq', 'tp')
- clipped_key_weight: bfloat16 [8192, 1024], P('seq')
The draws below stay inside these ranges and needn't reach their ends.
All inputs are finite; a program needn't handle non-finite values.
Results may differ from the reference program's by a relative error of at most 0.004.
Values may be sent and summed in bfloat16 or wider, within the bound.
A program may use at most 64 MiB of HBM per device.

```python
import math
import jax
import jax.numpy as jnp
from jax import lax

MODEL_WIDTH = 8192
QUERY_HEADS = 64
KEY_VALUE_HEADS = 8
HEAD_SIZE = 128
SEQUENCE_LENGTH = 2048


def random_key_table(key):
    gaussian_sample = jnp.clip(jax.random.normal(jax.random.fold_in(key, 71), (SEQUENCE_LENGTH, KEY_VALUE_HEADS, HEAD_SIZE), jnp.float32), -5.0, 5.0)
    return gaussian_sample


def draw_keys(key, part):
    return random_key_table(key).reshape(SEQUENCE_LENGTH, KEY_VALUE_HEADS * HEAD_SIZE).astype(jnp.bfloat16)


def draw_queries(key, part):
    head_scale = jnp.exp(jax.random.uniform(jax.random.fold_in(key, 72), (QUERY_HEADS,), jnp.float32, math.log(0.3), math.log(3.0)))
    gaussian_sample = jnp.clip(jax.random.normal(jax.random.fold_in(key, 73), (SEQUENCE_LENGTH, QUERY_HEADS, HEAD_SIZE), jnp.float32), -5.0, 5.0)
    gaussian_sample = gaussian_sample * head_scale[None, :, None]
    return gaussian_sample.reshape(SEQUENCE_LENGTH, QUERY_HEADS * HEAD_SIZE).astype(jnp.bfloat16)


def levels(rng, dims, shards, least, top_value):
    loudness = 1.0
    for position, parts in shards:
        draws = jax.random.uniform(jax.random.fold_in(jax.random.fold_in(rng, 6), position), (parts,), jnp.float32, least / len(shards), top_value / len(shards))
        loudness = loudness * jnp.repeat(jnp.exp(draws), dims[position] // parts).reshape((-1,) + (1,) * (len(dims) - 1 - position))
    return loudness


def centred(own_key, dims, width, bound, pieces=(), held_as=jnp.bfloat16):
    factor_of = levels(own_key, dims, pieces, -0.22, 0.18) if pieces else 1.0
    values = jax.random.normal(own_key, dims, jnp.float32) * width * factor_of
    return jnp.minimum(jnp.maximum(values, -bound), bound).astype(held_as)


def setup_inputs(seed: int = 0) -> dict:
    arg_keys = jax.random.split(jax.random.key(seed), 6)
    return {
        "queries": draw_queries(jax.random.fold_in(arg_keys[5], 71), 0),
        "keys": draw_keys(jax.random.fold_in(arg_keys[5], 71), 0),
        "values": centred(arg_keys[2], (SEQUENCE_LENGTH, KEY_VALUE_HEADS * HEAD_SIZE), 1.0, 6.0, ((0, 8), (1, 4))),
        "w_query": centred(arg_keys[3], (MODEL_WIDTH, QUERY_HEADS * HEAD_SIZE), MODEL_WIDTH ** -0.5, 0.0625, ((0, 8), (1, 4))),
        "key_weight": centred(arg_keys[4], (MODEL_WIDTH, KEY_VALUE_HEADS * HEAD_SIZE), MODEL_WIDTH ** -0.5, 0.0625, ((0, 8),)),
    }


clip_threshold = 10.0

def reference(queries, keys, values, w_query, key_weight):
    group_size = QUERY_HEADS // KEY_VALUE_HEADS
    block_rows = math.gcd(SEQUENCE_LENGTH, 512)
    inv_sqrt = HEAD_SIZE ** (-0.5)
    query_heads_view = jnp.moveaxis(queries.reshape(SEQUENCE_LENGTH, KEY_VALUE_HEADS, group_size, HEAD_SIZE), 1, 0)
    key_heads_view = jnp.moveaxis(keys.reshape(SEQUENCE_LENGTH, KEY_VALUE_HEADS, HEAD_SIZE), 1, 0)
    value_heads_view = jnp.moveaxis(values.reshape(SEQUENCE_LENGTH, KEY_VALUE_HEADS, HEAD_SIZE), 1, 0)
    key_positions = jnp.arange(SEQUENCE_LENGTH, dtype=jnp.int32)

    def one_head(operands):
        head_queries, head_keys, head_values = operands
        keys_wide = head_keys.astype(jnp.float32)
        values_wide = head_values.astype(jnp.float32)

        def one_block(running, block_index):
            block_queries = lax.dynamic_slice_in_dim(head_queries, block_index * block_rows, block_rows, 0).astype(jnp.float32)
            scores = jnp.einsum('bgd,nd->bgn', block_queries, keys_wide) * inv_sqrt
            query_positions = block_index * block_rows + jnp.arange(block_rows, dtype=jnp.int32)
            visible = (query_positions[:, None] >= key_positions[None, :])[:, None, :]
            masked = jnp.where(visible, scores, jnp.float32(-1e+30))
            row_max = masked.max(-1)
            expo = jnp.where(visible, jnp.exp(masked - row_max[..., None]), jnp.float32(0.0))
            totals = expo.sum(-1)
            probs = lax.optimization_barrier(expo.astype(jnp.bfloat16)).astype(jnp.float32)
            mixed = jnp.einsum('bgn,nd->bgd', probs, values_wide) / totals[..., None]
            return (jnp.maximum(running, masked.max(axis=(0, 2))), mixed.astype(jnp.bfloat16))
        head_max, block_out = lax.scan(one_block, jnp.full((group_size,), -1e+30, jnp.float32), jnp.arange(SEQUENCE_LENGTH // block_rows, dtype=jnp.int32))
        return (head_max, block_out.reshape(SEQUENCE_LENGTH, group_size, HEAD_SIZE))
    head_max, outputs = lax.map(one_head, (query_heads_view, key_heads_view, value_heads_view))
    attended = jnp.moveaxis(outputs, 0, 1).reshape(SEQUENCE_LENGTH, QUERY_HEADS * HEAD_SIZE)
    head_logit_maxima = head_max.reshape(QUERY_HEADS)
    gamma = clip_threshold / jnp.maximum(head_logit_maxima, clip_threshold)
    clip_logits = clip_threshold / jnp.maximum(head_logit_maxima.reshape(KEY_VALUE_HEADS, group_size).max(1), clip_threshold)
    query_factor = gamma / jnp.sqrt(jnp.repeat(clip_logits, group_size))
    w_query_clipped = (w_query.astype(jnp.float32).reshape(MODEL_WIDTH, QUERY_HEADS, HEAD_SIZE) * query_factor[None, :, None]).reshape(MODEL_WIDTH, QUERY_HEADS * HEAD_SIZE).astype(jnp.bfloat16)
    clipped_key_weight = (key_weight.astype(jnp.float32).reshape(MODEL_WIDTH, KEY_VALUE_HEADS, HEAD_SIZE) * jnp.sqrt(clip_logits)[None, :, None]).reshape(MODEL_WIDTH, KEY_VALUE_HEADS * HEAD_SIZE).astype(jnp.bfloat16)
    return (attended, head_logit_maxima, w_query_clipped, clipped_key_weight)
```

```python
import functools
import math

import jax
import jax.numpy as jnp
from jax import lax
from jax.experimental import pallas as pl
from jax.experimental.pallas import tpu as pltpu
from jax.sharding import PartitionSpec as P

HEAD_SIZE = 128
LANES = 128

clip_threshold = 10.0
HEADS_PER_STEP = 8
MESH = pl.DeviceIdType.MESH


def grid_of(n):
    columns = max(d for d in range(1, n + 1) if n % d == 0 and d * d <= n)
    return n // columns, columns


def attend_kernel(
    n, tp_n, heads, kv_heads, rows,
    q_hbm, k_hbm, v_hbm,
    o_ref, qf_ref, kf_ref, hm_ref,
    qv, kb, vb, kt, acc, mrun, mxl, mxb, gml, gmb,
    lq, lkv, k_recv, v_recv, k_send, v_send, mx_recv, mx_send, gm_recv, gm_send,
):
    group = heads // kv_heads
    nz, nx = grid_of(n)
    me = lax.axis_index("seq")
    tp = lax.axis_index("tp")
    z, x = lax.div(me, nx), lax.rem(me, nx)

    def head_cols(h):
        return pl.ds(h * HEAD_SIZE, HEAD_SIZE)

    kv_copies = []
    for g in range(kv_heads):
        kv_copies.append(pltpu.make_async_copy(k_hbm.at[:, head_cols(g)], kb.at[me, g], lkv.at[0, g]))
        kv_copies.append(pltpu.make_async_copy(v_hbm.at[:, head_cols(g)], vb.at[me, g], lkv.at[1, g]))
    for copy in kv_copies:
        copy.start()
    q_copies = [
        pltpu.make_async_copy(q_hbm.at[:, head_cols(h)], qv.at[h], lq.at[h]) for h in range(heads)
    ]
    for copy in q_copies:
        copy.start()

    barrier = pltpu.get_barrier_semaphore()
    for d in range(1, n):
        pl.semaphore_signal(
            barrier, inc=1, device_id={"seq": lax.rem(me + d, n)}, device_id_type=MESH
        )
    for d in range(1, tp_n):
        pl.semaphore_signal(
            barrier, inc=1, device_id={"tp": lax.rem(tp + d, tp_n)}, device_id_type=MESH
        )
    for copy in kv_copies:
        copy.wait()
    pl.semaphore_wait(barrier, n - 1 + tp_n - 1)

    def piece(kind, block, way, target):
        buf, send, recv = ((kb, k_send, k_recv), (vb, v_send, v_recv))[kind]
        return pltpu.make_async_remote_copy(
            src_ref=buf.at[block], dst_ref=buf.at[block],
            send_sem=send.at[way, block], recv_sem=recv.at[block],
            device_id={"seq": target}, device_id_type=MESH,
        )

    def each_send(kind, row, col, act):
        block = row * nx + col

        @pl.when((col == x) & (z + 1 < nz))
        def _():
            act(piece(kind, block, 0, lax.rem(me + nx, n)))

        @pl.when((col <= x) & (x + 1 < nx))
        def _():
            act(piece(kind, block, 1, lax.rem(me + 1, n)))

        @pl.when((col >= x) & (x > 0) & (row < z))
        def _():
            act(piece(kind, block, 2, lax.rem(me + n - 1, n)))

    start = lambda copy: copy.start()
    for kind in range(2):
        each_send(kind, z, x, start)
    for copy in q_copies:
        copy.wait()

    scale = HEAD_SIZE ** (-0.5)
    to_exp2 = scale * math.log2(math.e)
    ones = jnp.ones((rows, LANES), jnp.bfloat16)

    def wide(a):
        return jnp.concatenate([a] * (rows // LANES), axis=1)

    def widest(s):
        top = s[:, :LANES]
        for i in range(1, rows // LANES):
            top = jnp.maximum(top, s[:, i * LANES:(i + 1) * LANES])
        return jnp.broadcast_to(jnp.max(top, axis=1, keepdims=True), (rows, LANES))

    steps = heads // HEADS_PER_STEP

    def place(t):
        u = jnp.maximum(t - x - 1, 0)
        first = t <= x
        w = jnp.maximum(u - 1, 0)
        k = 1 + lax.div(w, nx)
        j = lax.rem(w, nx) + jnp.where(k == z, 1, 0)
        up = jnp.where(u == 0, 1, jnp.where(j == 0, k + 1, k))
        left = jnp.where(u == 0, 0, j)
        row = jnp.where(first, z, z - up)
        col = jnp.where(first, x - t, lax.rem(x + nx - left, nx))
        return row, col

    def take(kind, t):
        row, col = place(t)
        piece(kind, row * nx + col, 0, lax.rem(me + 1, n)).wait_recv()
        each_send(kind, row, col, start)

    def attend(block, t, own):
        for g in range(kv_heads):
            kt[g] = kb[block, g].T

        @pl.loop(0, steps)
        def _(step):
            for i in range(HEADS_PER_STEP):
                h = step * HEADS_PER_STEP + i
                g = lax.div(h, group)
                s = jnp.dot(qv[h], kt[g], preferred_element_type=jnp.float32)
                if own:
                    r = lax.broadcasted_iota(jnp.int32, (rows, rows), 0)
                    c = lax.broadcasted_iota(jnp.int32, (rows, rows), 1)
                    s = jnp.where(r >= c, s, jnp.float32(-1e30))
                v_ones = jnp.concatenate([vb[block, g], ones], axis=1)
                if own:
                    top = widest(s)
                    p = jnp.exp2((s - wide(top)) * to_exp2).astype(jnp.bfloat16)
                    acc[h] = jnp.dot(p, v_ones, preferred_element_type=jnp.float32)
                else:
                    old = mrun[h]
                    top = jnp.maximum(old, widest(s))
                    p = jnp.exp2((s - wide(top)) * to_exp2).astype(jnp.bfloat16)
                    keep = jnp.exp2((old - top) * to_exp2)
                    acc[h] = acc[h] * jnp.concatenate([keep, keep], axis=1) + jnp.dot(
                        p, v_ones, preferred_element_type=jnp.float32
                    )
                mrun[h] = top

            @pl.when((step == steps // 2 - 1) & (t < me))
            def _():
                take(0, t + 1)

            @pl.when((step == steps - 1) & (t < me))
            def _():
                take(1, t + 1)

    attend(me, 0, True)

    def one_block(t, carry):
        row, col = place(t)
        attend(row * nx + col, t, False)
        return carry

    lax.fori_loop(1, me + 1, one_block, 0)

    sub = lax.broadcasted_iota(jnp.int32, (heads, LANES), 0)
    local = jnp.zeros((heads, LANES), jnp.float32)
    for h in range(heads):
        local = jnp.where(sub == h, jnp.max(mrun[h], axis=0, keepdims=True), local)
    mxl[...] = local

    def mx_copy(d):
        return pltpu.make_async_remote_copy(
            src_ref=mxl, dst_ref=mxb.at[d - 1], send_sem=mx_send.at[d - 1],
            recv_sem=mx_recv.at[d - 1], device_id={"seq": lax.rem(me + d, n)}, device_id_type=MESH,
        )

    for d in range(1, n):
        mx_copy(d).start()

    for h in range(heads):
        a = acc[h]
        o_ref[:, h * HEAD_SIZE:(h + 1) * HEAD_SIZE] = (a[:, :HEAD_SIZE] / a[:, HEAD_SIZE:]).astype(jnp.bfloat16)

    top = local
    for d in range(1, n):
        mx_copy(d).wait_recv()
        top = jnp.maximum(top, mxb[d - 1])
    top = top * scale
    gsub = lax.broadcasted_iota(jnp.int32, (8, LANES), 0)
    gtop = jnp.zeros((8, LANES), jnp.float32)
    for g in range(kv_heads):
        gtop = jnp.where(
            gsub == g, jnp.max(top[g * group:(g + 1) * group], axis=0, keepdims=True), gtop
        )
    gml[...] = gtop

    def gm_copy(d):
        return pltpu.make_async_remote_copy(
            src_ref=gml, dst_ref=gmb.at[d - 1], send_sem=gm_send.at[d - 1],
            recv_sem=gm_recv.at[d - 1], device_id={"tp": lax.rem(tp + d, tp_n)}, device_id_type=MESH,
        )

    for d in range(1, tp_n):
        gm_copy(d).start()

    lane = lax.broadcasted_iota(jnp.int32, (1, LANES), 1)
    hm = jnp.zeros((1, LANES), jnp.float32)
    gamma = clip_threshold / jnp.maximum(top, clip_threshold)
    clip = clip_threshold / jnp.maximum(gtop, clip_threshold)
    for h in range(heads):
        hm = jnp.where(lane == h, top[h:h + 1], hm)
        g = h // group
        qf_ref[:, h * HEAD_SIZE:(h + 1) * HEAD_SIZE] = gamma[h:h + 1] / jnp.sqrt(clip[g:g + 1])
    hm_ref[...] = hm

    def put_key_factors(owner, factors):
        for g in range(kv_heads):
            at = pl.multiple_of((owner * kv_heads + g) * HEAD_SIZE, HEAD_SIZE)
            kf_ref[:, pl.ds(at, HEAD_SIZE)] = jnp.sqrt(factors[g:g + 1])

    put_key_factors(tp, clip)
    for d in range(1, tp_n):
        gm_copy(d).wait_recv()
        put_key_factors(
            lax.rem(tp + tp_n - d, tp_n), clip_threshold / jnp.maximum(gmb[d - 1], clip_threshold)
        )

    def sent_row(row, carry):
        def sent_col(col, carry):
            @pl.when((row < z) | (col <= x))
            def _():
                for kind in range(2):
                    each_send(kind, row, col, lambda copy: copy.wait_send())

            return carry

        return lax.fori_loop(0, nx, sent_col, carry)

    lax.fori_loop(0, z + 1, sent_row, 0)
    for d in range(1, n):
        mx_copy(d).wait_send()
    for d in range(1, tp_n):
        gm_copy(d).wait_send()


CHUNKS = 8


def finish_kernel(heads, a_ref, qf_ref, kf_ref, hm_ref, w_ref, kw_ref, a_hbm, top_ref, w_hbm, kw_hbm, wb, kwb, sem):
    copies = [pltpu.make_async_copy(a_ref, a_hbm, sem.at[0])]
    copies[0].start()
    for src, factor, buf, dst, first in ((w_ref, qf_ref, wb, w_hbm, 1), (kw_ref, kf_ref, kwb, kw_hbm, 1 + CHUNKS)):
        size = src.shape[0] // CHUNKS
        for i in range(CHUNKS):
            rows = pl.ds(i * size, size)
            buf[rows, :] = (src[rows, :].astype(jnp.float32) * factor[...]).astype(jnp.bfloat16)
            copy = pltpu.make_async_copy(buf.at[rows], dst.at[rows], sem.at[first + i])
            copy.start()
            copies.append(copy)
    top_ref[...] = hm_ref[0, :heads]
    for copy in copies:
        copy.wait()


def shards(n, tp_n, queries, keys, values, w_query, key_weight):
    rows = queries.shape[0]
    heads = queries.shape[1] // HEAD_SIZE
    kv_heads = keys.shape[1] // HEAD_SIZE
    vmem = pl.BlockSpec(memory_space=pltpu.VMEM)
    dma = pltpu.SemaphoreType.DMA
    attended, q_factor, k_factor, maxima = pl.pallas_call(
        functools.partial(attend_kernel, n, tp_n, heads, kv_heads, rows),
        name="attend",
        out_shape=(
            jax.ShapeDtypeStruct(queries.shape, jnp.bfloat16),
            jax.ShapeDtypeStruct((1, heads * HEAD_SIZE), jnp.float32),
            jax.ShapeDtypeStruct((1, key_weight.shape[1]), jnp.float32),
            jax.ShapeDtypeStruct((1, LANES), jnp.float32),
        ),
        in_specs=[pl.BlockSpec(memory_space=pltpu.HBM)] * 3,
        out_specs=(vmem, vmem, vmem, vmem),
        scratch_shapes=[
            pltpu.VMEM((heads, rows, HEAD_SIZE), jnp.bfloat16),
            pltpu.VMEM((n, kv_heads, rows, HEAD_SIZE), jnp.bfloat16),
            pltpu.VMEM((n, kv_heads, rows, HEAD_SIZE), jnp.bfloat16),
            pltpu.VMEM((kv_heads, HEAD_SIZE, rows), jnp.bfloat16),
            pltpu.VMEM((heads, rows, 2 * HEAD_SIZE), jnp.float32),
            pltpu.VMEM((heads, rows, LANES), jnp.float32),
            pltpu.VMEM((heads, LANES), jnp.float32),
            pltpu.VMEM((n - 1, heads, LANES), jnp.float32),
            pltpu.VMEM((8, LANES), jnp.float32),
            pltpu.VMEM((tp_n - 1, 8, LANES), jnp.float32),
            dma((heads,)),
            dma((2, kv_heads)),
            dma((n,)),
            dma((n,)),
            dma((3, n)),
            dma((3, n)),
            dma((n - 1,)),
            dma((n - 1,)),
            dma((tp_n - 1,)),
            dma((tp_n - 1,)),
        ],
        compiler_params=pltpu.CompilerParams(
            collective_id=0, has_side_effects=True, vmem_limit_bytes=32 * 1024 * 1024
        ),
        cost_estimate=pl.CostEstimate(
            flops=4 * rows * rows * n * heads * HEAD_SIZE,
            bytes_accessed=4 * rows * heads * HEAD_SIZE,
            transcendentals=rows * rows * n * heads,
        ),
    )(*(pltpu.with_memory_space_constraint(a, pltpu.HBM) for a in (queries, keys, values)))
    hbm = pl.BlockSpec(memory_space=pltpu.HBM)
    return pl.pallas_call(
        functools.partial(finish_kernel, heads),
        name="finish",
        out_shape=(
            jax.ShapeDtypeStruct(queries.shape, jnp.bfloat16),
            jax.ShapeDtypeStruct((heads,), jnp.float32),
            jax.ShapeDtypeStruct(w_query.shape, jnp.bfloat16),
            jax.ShapeDtypeStruct(key_weight.shape, jnp.bfloat16),
        ),
        in_specs=[vmem] * 6,
        out_specs=(hbm, vmem, hbm, hbm),
        scratch_shapes=[
            pltpu.VMEM(w_query.shape, jnp.bfloat16),
            pltpu.VMEM(key_weight.shape, jnp.bfloat16),
            dma((1 + 2 * CHUNKS,)),
        ],
        compiler_params=pltpu.CompilerParams(vmem_limit_bytes=24 * 1024 * 1024),
        cost_estimate=pl.CostEstimate(
            flops=w_query.size + key_weight.size,
            bytes_accessed=4 * (w_query.size + key_weight.size),
            transcendentals=0,
        ),
    )(attended, q_factor, k_factor, maxima, w_query, key_weight)


def solution(mesh):
    in_specs = (P("seq", "tp"), P("seq", "tp"), P("seq", "tp"), P("seq", "tp"), P("seq", None))
    out_specs = (P("seq", "tp"), P("tp"), P("seq", "tp"), P("seq", None))
    body = functools.partial(shards, mesh.shape["seq"], mesh.shape["tp"])
    return jax.shard_map(body, mesh=mesh, in_specs=in_specs, out_specs=out_specs, check_vma=False)
```

```python
import functools
import math

import jax
import jax.numpy as jnp
from jax import lax
from jax.experimental import pallas as pl
from jax.experimental.pallas import tpu as pltpu
from jax.sharding import PartitionSpec as P

HEAD_SIZE = 128
LANES = 128

clip_threshold = 10.0
WINDOW = 7
UP, RIGHT, LEFT = range(3)
MESH = pl.DeviceIdType.MESH


def grid_of(n):
    columns = max(d for d in range(1, n + 1) if n % d == 0 and d * d <= n)
    return n // columns, columns


def attend_kernel(
    n, tp_n, heads, kv_heads, rows, slots,
    q_hbm, k_hbm, v_hbm, w_hbm, kw_hbm,
    acc, qf_ref, kf_ref, hm_ref, w_ref, kw_ref,
    qv, kv, kt, mrun, pb, kp, mxl, mxb,
    lq, lkv, lw, recv, send, mx_recv, mx_send,
):
    group = heads // kv_heads
    nz, nx = grid_of(n)
    me = lax.axis_index("seq")
    tp = lax.axis_index("tp")
    z, x = lax.div(me, nx), lax.rem(me, nx)
    everyone = n * tp_n
    mine = me * tp_n + tp
    alone = slots == n - 1

    def head_cols(h):
        return pl.ds(h * HEAD_SIZE, HEAD_SIZE)

    def peer(d):
        other = lax.rem(mine + d, everyone)
        return {"seq": lax.div(other, tp_n), "tp": lax.rem(other, tp_n)}

    for g in range(kv_heads):
        for kind, hbm in enumerate((k_hbm, v_hbm)):
            pltpu.make_async_copy(hbm.at[:, head_cols(g)], kv.at[me, kind, g], lkv).start()
    q_copy = pltpu.make_async_copy(q_hbm, qv, lq)
    q_copy.start()

    barrier = pltpu.get_barrier_semaphore()

    @pl.loop(1, everyone)
    def _(d):
        pl.semaphore_signal(barrier, inc=1, device_id=peer(d), device_id_type=MESH)

    pltpu.make_async_copy(kv.at[me], kv.at[me], lkv).wait()
    pl.semaphore_wait(barrier, everyone - 1)

    def piece(kind, block, g, way, target):
        ref = kv.at[block, kind, g]
        return pltpu.make_async_remote_copy(
            src_ref=ref, dst_ref=ref, send_sem=send.at[way, block], recv_sem=recv.at[kind, block, g],
            device_id={"seq": target}, device_id_type=MESH,
        )

    def routes(kind, row, col):
        up = col == x
        right = col <= x
        if kind == 1:
            up = up | ((row == z) & (col == x - 1))
            right = right & jnp.logical_not((row == z - 1) & (col == x))
        return (
            up & (z + 1 < nz),
            right & (x + 1 < nx),
            (col >= x) & (x > 0) & (row < z),
        )

    towards = (lax.rem(me + nx, n), lax.rem(me + 1, n), lax.rem(me + n - 1, n))

    def each_send(kind, g, row, col, ways=(UP, RIGHT, LEFT)):
        on = routes(kind, row, col)
        for way in ways:
            @pl.when(on[way])
            def _():
                piece(kind, row * nx + col, g, way, towards[way]).start()

    def await_sent(row, col):
        block = row * nx + col
        for way, (key, value) in enumerate(zip(routes(0, row, col), routes(1, row, col))):
            def done(ref):
                pltpu.make_async_remote_copy(
                    src_ref=ref, dst_ref=ref, send_sem=send.at[way, block], recv_sem=recv.at[0, block, 0],
                    device_id={"seq": towards[way]}, device_id_type=MESH,
                ).wait_send()

            @pl.when(key & value)
            def _():
                done(kv.at[block])

            @pl.when(key & jnp.logical_not(value))
            def _():
                done(kv.at[block, 0])

            @pl.when(value & jnp.logical_not(key))
            def _():
                done(kv.at[block, 1])

    for g in range(kv_heads):
        each_send(0, g, z, x, (UP, RIGHT))
    each_send(1, 0, z, x, (UP, RIGHT))

    def rest_of_own():
        for g in range(1, kv_heads):
            each_send(1, g, z, x, (UP, RIGHT))

    @pl.when(z == 0)
    def _():
        rest_of_own()

    q_copy.wait()

    scale = HEAD_SIZE ** (-0.5)
    to_exp2 = scale * math.log2(math.e)
    ones = jnp.ones((rows, LANES), jnp.bfloat16)

    def wide(a):
        return jnp.concatenate([a] * (rows // LANES), axis=1)

    def widest(s):
        top = s[:, :LANES]
        for i in range(1, rows // LANES):
            top = jnp.maximum(top, s[:, i * LANES:(i + 1) * LANES])
        return jnp.broadcast_to(jnp.max(top, axis=1, keepdims=True), (rows, LANES))

    def place(t):
        below = jnp.where(z > 0, 1, 0)
        along = t - below
        beside = (along >= 1) & (along <= x)
        u = jnp.where(t == below, 0, jnp.maximum(t - x - 1, 0))
        w = jnp.maximum(u - 1, 0)
        k = 1 + lax.div(w, nx)
        j = lax.rem(w, nx) + jnp.where(k == z, 1, 0)
        up = jnp.where(u == 0, 1, jnp.where(j == 0, k + 1, k))
        left = jnp.where(u == 0, 0, j)
        row = jnp.where(beside, z, z - up)
        col = jnp.where(beside, x - along, lax.rem(x + nx - left, nx))
        column = t <= z
        beside = (t > z) & (t <= z + x)
        v = jnp.maximum(t - z - x - 1, 0)
        inner_row = jnp.where(column, z - t, jnp.where(beside, z, z - 1 - lax.div(v, nx - 1)))
        inner_col = jnp.where(
            column, x, jnp.where(beside, x - t + z, lax.rem(x + nx - 1 - lax.rem(v, nx - 1), nx))
        )
        edge = x + 1 == nx
        return jnp.where(edge, row, inner_row), jnp.where(edge, col, inner_col)

    def take(kind, g, t):
        row, col = place(t)
        piece(kind, row * nx + col, g, RIGHT, towards[RIGHT]).wait_recv()
        each_send(kind, g, row, col)

    def own_part(g):
        kt[g] = kv[me, 0, g].T
        r = lax.broadcasted_iota(jnp.int32, (rows, rows), 0)
        c = lax.broadcasted_iota(jnp.int32, (rows, rows), 1)
        for i in range(group):
            h = g * group + i
            s = jnp.dot(qv[:, h * HEAD_SIZE:(h + 1) * HEAD_SIZE], kt[g], preferred_element_type=jnp.float32)
            s = jnp.where(r >= c, s, jnp.float32(-1e30))
            top = widest(s)
            mrun[h] = top
            p = jnp.exp2((s - wide(top)) * to_exp2).astype(jnp.bfloat16)
            v_ones = jnp.concatenate([kv[me, 1, g], ones], axis=1)
            acc[h] = jnp.dot(p, v_ones, preferred_element_type=jnp.float32)

    def score_part(g, t):
        row, col = place(t)
        kt[g] = kv[row * nx + col, 0, g].T
        slot = lax.rem(t - 1, slots)
        for i in range(group):
            h = g * group + i
            s = jnp.dot(qv[:, h * HEAD_SIZE:(h + 1) * HEAD_SIZE], kt[g], preferred_element_type=jnp.float32)
            old = mrun[h]
            top = jnp.maximum(old, widest(s))
            mrun[h] = top
            kp[slot, h] = jnp.exp2((old - top) * to_exp2)
            pb[slot, h] = jnp.exp2((s - wide(top)) * to_exp2).astype(jnp.bfloat16)

    def value_part(g, t):
        row, col = place(t)
        block = row * nx + col
        slot = lax.rem(t - 1, slots)
        for i in range(group):
            h = g * group + i
            v_ones = jnp.concatenate([kv[block, 1, g], ones], axis=1)
            keep = kp[slot, h]
            acc[h] = acc[h] * jnp.concatenate([keep, keep], axis=1) + jnp.dot(
                pb[slot, h], v_ones, preferred_element_type=jnp.float32
            )

    weight_copies = [
        pltpu.make_async_copy(w_hbm, w_ref, lw.at[0]), pltpu.make_async_copy(kw_hbm, kw_ref, lw.at[1])
    ]
    for copy in weight_copies:
        copy.start()

    for g in range(kv_heads):
        own_part(g)

    def score_step(t):
        row, col = place(t)
        for g in range(kv_heads):
            take(0, g, t)
            if g == kv_heads - 1:
                @pl.when((row == 0) & (col == x))
                def _():
                    rest_of_own()
            score_part(g, t)

    last = z + 1 == nz

    def early(t):
        column = place(t)[1] == x
        soon = jnp.where(x + 1 < nx, (t >= 2) & (t < z), t == 1)
        return column & jnp.where(last, soon, z >= 1)

    def ahead(t):
        column = place(t)[1] == x
        return last & column & (t > 2) & (t <= me) & jnp.logical_not(early(t))

    def take_values(t):
        for g in range(kv_heads):
            take(1, g, t)

    def value_step(t):
        if alone:
            @pl.when(last & jnp.logical_not(early(t) | ahead(t)))
            def _():
                take_values(t)

            @pl.when(ahead(t + 2))
            def _():
                take_values(t + 2)
        else:
            take_values(t)

        for g in range(kv_heads):
            value_part(g, t)
        @pl.when(t > 2)
        def _():
            await_sent(*place(t - 2))

    lane = lax.broadcasted_iota(jnp.int32, (1, LANES), 1)
    def mx_copy(d, owner):
        return pltpu.make_async_remote_copy(
            src_ref=mxl, dst_ref=mxb.at[owner], send_sem=mx_send,
            recv_sem=mx_recv, device_id=peer(d), device_id_type=MESH,
        )

    def send_maxima():
        local = jnp.full((1, LANES), -1e30, jnp.float32)
        for h in range(heads):
            local = jnp.where(lane == h, jnp.max(mrun[h], axis=0, keepdims=True), local)
        mxl[...] = local
        mxb[mine] = local

        @pl.loop(1, everyone)
        def _(d):
            mx_copy(d, mine).start()

    if alone:
        @pl.loop(1, me + 1)
        def _(t):
            @pl.when(t == me)
            def _():
                @pl.loop(1, me + 1)
                def _(s):
                    @pl.when(early(s))
                    def _():
                        take_values(s)

            score_step(t)

        send_maxima()

        @pl.loop(1, jnp.where(last, 1, me + 1))
        def _(t):
            @pl.when(jnp.logical_not(early(t)))
            def _():
                take_values(t)

        @pl.loop(1, me + 1)
        def _(t):
            value_step(t)
    else:
        @pl.loop(1, me + 1)
        def _(t):
            score_step(t)
            value_step(t)

        send_maxima()

    others = mxb.at[pl.ds(0, everyone - 1)]
    exchange = pltpu.make_async_remote_copy(
        src_ref=others, dst_ref=others, send_sem=mx_send, recv_sem=mx_recv,
        device_id=peer(1), device_id_type=MESH,
    )
    exchange.wait_recv()

    def widest_lanes(a, keep):
        return jnp.broadcast_to(
            jnp.max(jnp.where(keep, a, -1e30), axis=1, keepdims=True), (1, LANES)
        )

    def clip_of(top):
        return clip_threshold / jnp.maximum(top * scale, clip_threshold)

    def shard_top(owner):
        top = mxb[owner]
        for i in range(1, n):
            top = jnp.maximum(top, mxb[i * tp_n + owner])
        return top

    def in_group(g):
        return (lane >= g * group) & (lane < (g + 1) * group)

    top = shard_top(tp)
    hm_ref[...] = top * scale
    clip = [clip_of(widest_lanes(top, in_group(g))) for g in range(kv_heads)]
    for h in range(heads):
        qf_ref[:, h * HEAD_SIZE:(h + 1) * HEAD_SIZE] = clip_of(
            widest_lanes(top, lane == h)
        ) / jnp.sqrt(clip[h // group])
    for owner in range(tp_n):
        other = shard_top(owner)
        for g in range(kv_heads):
            at = (owner * kv_heads + g) * HEAD_SIZE
            kf_ref[:, at:at + HEAD_SIZE] = jnp.sqrt(clip_of(widest_lanes(other, in_group(g))))

    await_sent(z, x)

    @pl.loop(jnp.maximum(me - 1, 1), me + 1)
    def _(t):
        await_sent(*place(t))

    for copy in weight_copies:
        copy.wait()

    exchange.wait_send()


CHUNKS = 8


def finish_kernel(heads, acc, qf_ref, kf_ref, hm_ref, w_ref, kw_ref, a_hbm, top_ref, w_hbm, kw_hbm, wb, kwb, ab, sem):
    for at, src, factor, buf, dst in ((0, w_ref, qf_ref, wb, w_hbm), (1, kw_ref, kf_ref, kwb, kw_hbm)):
        size = src.shape[0] // CHUNKS
        for i in range(CHUNKS):
            rows = pl.ds(i * size, size)
            buf[rows, :] = (src[rows, :].astype(jnp.float32) * factor[...]).astype(jnp.bfloat16)
            pltpu.make_async_copy(buf.at[rows], dst.at[rows], sem.at[at]).start()
    top_ref[...] = hm_ref[0, :heads]
    for h in range(heads):
        cols = slice(h * HEAD_SIZE, (h + 1) * HEAD_SIZE)
        a = acc[h]
        ab[:, cols] = (a[:, :HEAD_SIZE] / a[:, HEAD_SIZE:]).astype(jnp.bfloat16)
        pltpu.make_async_copy(ab.at[:, cols], a_hbm.at[:, cols], sem.at[2]).start()
    for at, buf, dst in ((0, wb, w_hbm), (1, kwb, kw_hbm), (2, ab, a_hbm)):
        pltpu.make_async_copy(buf, dst, sem.at[at]).wait()


def shards(n, tp_n, queries, keys, values, w_query, key_weight):
    rows = queries.shape[0]
    heads = queries.shape[1] // HEAD_SIZE
    kv_heads = keys.shape[1] // HEAD_SIZE
    slots = n - 1 if n - 1 <= WINDOW else 1
    everyone = n * tp_n
    vmem = pl.BlockSpec(memory_space=pltpu.VMEM)
    hbm = pl.BlockSpec(memory_space=pltpu.HBM)
    dma = pltpu.SemaphoreType.DMA
    acc, q_factor, k_factor, maxima, w_local, kw_local = pl.pallas_call(
        functools.partial(attend_kernel, n, tp_n, heads, kv_heads, rows, slots),
        name="attend",
        out_shape=(
            jax.ShapeDtypeStruct((heads, rows, 2 * HEAD_SIZE), jnp.float32),
            jax.ShapeDtypeStruct((1, heads * HEAD_SIZE), jnp.float32),
            jax.ShapeDtypeStruct((1, key_weight.shape[1]), jnp.float32),
            jax.ShapeDtypeStruct((1, LANES), jnp.float32),
            jax.ShapeDtypeStruct(w_query.shape, jnp.bfloat16),
            jax.ShapeDtypeStruct(key_weight.shape, jnp.bfloat16),
        ),
        in_specs=[hbm] * 5,
        out_specs=[vmem] * 6,
        scratch_shapes=[
            pltpu.VMEM((rows, heads * HEAD_SIZE), jnp.bfloat16),
            pltpu.VMEM((n, 2, kv_heads, rows, HEAD_SIZE), jnp.bfloat16),
            pltpu.VMEM((kv_heads, HEAD_SIZE, rows), jnp.bfloat16),
            pltpu.VMEM((heads, rows, LANES), jnp.float32),
            pltpu.VMEM((slots, heads, rows, rows), jnp.bfloat16),
            pltpu.VMEM((slots, heads, rows, LANES), jnp.float32),
            pltpu.VMEM((1, LANES), jnp.float32),
            pltpu.VMEM((everyone, 1, LANES), jnp.float32),
            dma,
            dma,
            dma((2,)),
            dma((2, n, kv_heads)),
            dma((3, n)),
            dma,
            dma,
        ],
        compiler_params=pltpu.CompilerParams(
            collective_id=0, has_side_effects=True, vmem_limit_bytes=36 * 1024 * 1024
        ),
        cost_estimate=pl.CostEstimate(
            flops=4 * rows * rows * n * heads * HEAD_SIZE,
            bytes_accessed=4 * rows * heads * HEAD_SIZE,
            transcendentals=rows * rows * n * heads,
        ),
    )(*(
        pltpu.with_memory_space_constraint(a, pltpu.HBM)
        for a in (queries, keys, values, w_query, key_weight)
    ))
    return pl.pallas_call(
        functools.partial(finish_kernel, heads),
        name="finish",
        out_shape=(
            jax.ShapeDtypeStruct(queries.shape, jnp.bfloat16),
            jax.ShapeDtypeStruct((heads,), jnp.float32),
            jax.ShapeDtypeStruct(w_query.shape, jnp.bfloat16),
            jax.ShapeDtypeStruct(key_weight.shape, jnp.bfloat16),
        ),
        in_specs=[vmem] * 6,
        out_specs=(hbm, vmem, hbm, hbm),
        scratch_shapes=[
            pltpu.VMEM(w_query.shape, jnp.bfloat16),
            pltpu.VMEM(key_weight.shape, jnp.bfloat16),
            pltpu.VMEM(queries.shape, jnp.bfloat16),
            dma((3,)),
        ],
        compiler_params=pltpu.CompilerParams(vmem_limit_bytes=24 * 1024 * 1024),
        cost_estimate=pl.CostEstimate(
            flops=w_query.size + key_weight.size,
            bytes_accessed=4 * (w_query.size + key_weight.size),
            transcendentals=0,
        ),
    )(acc, q_factor, k_factor, maxima, w_local, kw_local)


def solution(mesh):
    in_specs = (P("seq", "tp"), P("seq", "tp"), P("seq", "tp"), P("seq", "tp"), P("seq", None))
    out_specs = (P("seq", "tp"), P("tp"), P("seq", "tp"), P("seq", None))
    body = functools.partial(shards, mesh.shape["seq"], mesh.shape["tp"])
    return jax.shard_map(body, mesh=mesh, in_specs=in_specs, out_specs=out_specs, check_vma=False)
```

```python
import functools
import math

import jax
import jax.numpy as jnp
from jax import lax
from jax.experimental import pallas as pl
from jax.experimental.pallas import tpu as pltpu
from jax.sharding import PartitionSpec as P

HEAD_SIZE = 128
LANES = 128
SUMS = 16

clip_threshold = 10.0
WINDOW = 7
UP, RIGHT, LEFT = range(3)
MESH = pl.DeviceIdType.MESH


def grid_of(n):
    columns = max(d for d in range(1, n + 1) if n % d == 0 and d * d <= n)
    return n // columns, columns


def attend_kernel(
    n, tp_n, heads, kv_heads, rows, slots,
    q_hbm, k_hbm, v_hbm, w_hbm, kw_hbm,
    acc, qf_ref, kf_ref, hm_ref, w_ref, kw_ref,
    qv, kv, qt, vt, mrun, pb, kp, mxl, mxb,
    lq, lkv, lw, recv, send, mx_recv, mx_send,
):
    group = heads // kv_heads
    nz, nx = grid_of(n)
    me = lax.axis_index("seq")
    tp = lax.axis_index("tp")
    z, x = lax.div(me, nx), lax.rem(me, nx)
    everyone = n * tp_n
    mine = me * tp_n + tp
    alone = slots == n - 1

    def head_cols(h):
        return pl.ds(h * HEAD_SIZE, HEAD_SIZE)

    def peer(d):
        other = lax.rem(mine + d, everyone)
        return {"seq": lax.div(other, tp_n), "tp": lax.rem(other, tp_n)}

    for g in range(kv_heads):
        for kind, hbm in enumerate((k_hbm, v_hbm)):
            pltpu.make_async_copy(hbm.at[:, head_cols(g)], kv.at[me, kind, g], lkv).start()
    q_copy = pltpu.make_async_copy(q_hbm, qv, lq)
    q_copy.start()

    barrier = pltpu.get_barrier_semaphore()

    @pl.loop(1, everyone)
    def _(d):
        pl.semaphore_signal(barrier, inc=1, device_id=peer(d), device_id_type=MESH)

    pltpu.make_async_copy(kv.at[me], kv.at[me], lkv).wait()
    pl.semaphore_wait(barrier, everyone - 1)

    def piece(kind, block, g, way, target):
        ref = kv.at[block, kind, g]
        return pltpu.make_async_remote_copy(
            src_ref=ref, dst_ref=ref, send_sem=send.at[way, block], recv_sem=recv.at[kind, block, g],
            device_id={"seq": target}, device_id_type=MESH,
        )

    def routes(kind, row, col):
        up = col == x
        right = col <= x
        if kind == 1:
            up = up | ((row == z) & (col == x - 1))
            right = right & jnp.logical_not((row == z - 1) & (col == x))
        return (
            up & (z + 1 < nz),
            right & (x + 1 < nx),
            (col >= x) & (x > 0) & (row < z),
        )

    towards = (lax.rem(me + nx, n), lax.rem(me + 1, n), lax.rem(me + n - 1, n))

    def each_send(kind, g, row, col, ways=(UP, RIGHT, LEFT)):
        on = routes(kind, row, col)
        for way in ways:
            @pl.when(on[way])
            def _():
                piece(kind, row * nx + col, g, way, towards[way]).start()

    def await_sent(row, col):
        block = row * nx + col
        for way, (key, value) in enumerate(zip(routes(0, row, col), routes(1, row, col))):
            def done(ref):
                pltpu.make_async_remote_copy(
                    src_ref=ref, dst_ref=ref, send_sem=send.at[way, block], recv_sem=recv.at[0, block, 0],
                    device_id={"seq": towards[way]}, device_id_type=MESH,
                ).wait_send()

            @pl.when(key & value)
            def _():
                done(kv.at[block])

            @pl.when(key & jnp.logical_not(value))
            def _():
                done(kv.at[block, 0])

            @pl.when(value & jnp.logical_not(key))
            def _():
                done(kv.at[block, 1])

    for g in range(kv_heads):
        each_send(0, g, z, x, (UP, RIGHT))
    each_send(1, 0, z, x, (UP, RIGHT))

    def rest_of_own():
        for g in range(1, kv_heads):
            each_send(1, g, z, x, (UP, RIGHT))

    @pl.when(z == 0)
    def _():
        rest_of_own()

    q_copy.wait()

    scale = HEAD_SIZE ** (-0.5)
    to_exp2 = scale * math.log2(math.e)

    def place(t):
        below = jnp.where(z > 0, 1, 0)
        along = t - below
        beside = (along >= 1) & (along <= x)
        u = jnp.where(t == below, 0, jnp.maximum(t - x - 1, 0))
        w = jnp.maximum(u - 1, 0)
        k = 1 + lax.div(w, nx)
        j = lax.rem(w, nx) + jnp.where(k == z, 1, 0)
        up = jnp.where(u == 0, 1, jnp.where(j == 0, k + 1, k))
        left = jnp.where(u == 0, 0, j)
        row = jnp.where(beside, z, z - up)
        col = jnp.where(beside, x - along, lax.rem(x + nx - left, nx))
        return row, col

    def take(kind, g, t):
        row, col = place(t)
        piece(kind, row * nx + col, g, RIGHT, towards[RIGHT]).wait_recv()
        each_send(kind, g, row, col)

    def own_part(g):
        vt[g, :HEAD_SIZE] = kv[me, 1, g].T
        r = lax.broadcasted_iota(jnp.int32, (rows, rows), 0)
        c = lax.broadcasted_iota(jnp.int32, (rows, rows), 1)
        for i in range(group):
            h = g * group + i
            s = lax.dot_general(
                kv[me, 0, g], qv[:, h * HEAD_SIZE:(h + 1) * HEAD_SIZE], (((1,), (1,)), ((), ())),
                preferred_element_type=jnp.float32,
            )
            s = jnp.where(c >= r, s, jnp.float32(-1e30))
            top = jnp.max(s, axis=0, keepdims=True)
            mrun[h] = top
            pb[0, h] = jnp.exp2((s - top) * to_exp2).astype(jnp.bfloat16)
        for i in range(group):
            h = g * group + i
            acc[h] = jnp.dot(vt[g], pb[0, h], preferred_element_type=jnp.float32)

    def score_part(g, t):
        row, col = place(t)
        block = row * nx + col
        slot = lax.rem(t - 1, slots)
        for i in range(group):
            h = g * group + i
            s = jnp.dot(kv[block, 0, g], qt[h], preferred_element_type=jnp.float32)
            old = mrun[h]
            top = jnp.maximum(old, jnp.max(s, axis=0, keepdims=True))
            mrun[h] = top
            kp[slot, h] = jnp.exp2((old - top) * to_exp2)
            pb[slot, h] = jnp.exp2((s - top) * to_exp2).astype(jnp.bfloat16)

    def value_part(g, t):
        row, col = place(t)
        slot = lax.rem(t - 1, slots)
        vt[g, :HEAD_SIZE] = kv[row * nx + col, 1, g].T
        for i in range(group):
            h = g * group + i
            acc[h] = acc[h] * kp[slot, h] + jnp.dot(
                vt[g], pb[slot, h], preferred_element_type=jnp.float32
            )

    for g in range(kv_heads):
        vt[g, HEAD_SIZE:] = jnp.ones((SUMS, rows), jnp.bfloat16)

    weight_copies = [
        pltpu.make_async_copy(w_hbm, w_ref, lw.at[0]), pltpu.make_async_copy(kw_hbm, kw_ref, lw.at[1])
    ]
    for copy in weight_copies:
        copy.start()

    for g in range(kv_heads):
        own_part(g)
    for h in range(heads):
        qt[h] = qv[:, h * HEAD_SIZE:(h + 1) * HEAD_SIZE].T

    def score_step(t):
        row, col = place(t)
        for g in range(kv_heads):
            take(0, g, t)
            if g == kv_heads - 1:
                @pl.when((row == 0) & (col == x))
                def _():
                    rest_of_own()
            score_part(g, t)

    last = z + 1 == nz

    def early(t):
        column = place(t)[1] == x
        return column & jnp.where(last, (x + 1 == nx) & (t == 1), z >= 1)

    def ahead(t):
        column = place(t)[1] == x
        return last & column & (t > 1) & (t <= me)

    def take_values(t):
        for g in range(kv_heads):
            take(1, g, t)

    def value_step(t):
        if alone:
            @pl.when(last & jnp.logical_not(early(t) | ahead(t)))
            def _():
                take_values(t)

            @pl.when((t == 1) & ahead(2))
            def _():
                take_values(2)

            @pl.when(ahead(t + 2))
            def _():
                take_values(t + 2)
        else:
            take_values(t)

        for g in range(kv_heads):
            value_part(g, t)
        @pl.when(t > 2)
        def _():
            await_sent(*place(t - 2))

    lane = lax.broadcasted_iota(jnp.int32, (1, LANES), 1)
    def mx_copy(d, owner):
        return pltpu.make_async_remote_copy(
            src_ref=mxl, dst_ref=mxb.at[owner], send_sem=mx_send,
            recv_sem=mx_recv, device_id=peer(d), device_id_type=MESH,
        )

    def send_maxima():
        local = jnp.full((1, LANES), -1e30, jnp.float32)
        for h in range(heads):
            local = jnp.where(lane == h, jnp.max(mrun[h], axis=1, keepdims=True), local)
        mxl[...] = local
        mxb[mine] = local

        @pl.loop(1, everyone)
        def _(d):
            mx_copy(d, mine).start()

    if alone:
        @pl.loop(1, me + 1)
        def _(t):
            @pl.when(t == me)
            def _():
                @pl.loop(1, me + 1)
                def _(s):
                    @pl.when(early(s))
                    def _():
                        take_values(s)

            score_step(t)

        send_maxima()

        @pl.loop(1, jnp.where(last, 1, me + 1))
        def _(t):
            @pl.when(jnp.logical_not(early(t)))
            def _():
                take_values(t)

        @pl.loop(1, me + 1)
        def _(t):
            value_step(t)
    else:
        @pl.loop(1, me + 1)
        def _(t):
            score_step(t)
            value_step(t)

        send_maxima()

    others = mxb.at[pl.ds(0, everyone - 1)]
    exchange = pltpu.make_async_remote_copy(
        src_ref=others, dst_ref=others, send_sem=mx_send, recv_sem=mx_recv,
        device_id=peer(1), device_id_type=MESH,
    )
    exchange.wait_recv()

    def widest_lanes(a, keep):
        return jnp.broadcast_to(
            jnp.max(jnp.where(keep, a, -1e30), axis=1, keepdims=True), (1, LANES)
        )

    def clip_of(top):
        return clip_threshold / jnp.maximum(top * scale, clip_threshold)

    def shard_top(owner):
        top = mxb[owner]
        for i in range(1, n):
            top = jnp.maximum(top, mxb[i * tp_n + owner])
        return top

    def in_group(g):
        return (lane >= g * group) & (lane < (g + 1) * group)

    top = shard_top(tp)
    hm_ref[...] = top * scale
    clip = [clip_of(widest_lanes(top, in_group(g))) for g in range(kv_heads)]
    for h in range(heads):
        qf_ref[:, h * HEAD_SIZE:(h + 1) * HEAD_SIZE] = clip_of(
            widest_lanes(top, lane == h)
        ) / jnp.sqrt(clip[h // group])
    for owner in range(tp_n):
        other = shard_top(owner)
        for g in range(kv_heads):
            at = (owner * kv_heads + g) * HEAD_SIZE
            kf_ref[:, at:at + HEAD_SIZE] = jnp.sqrt(clip_of(widest_lanes(other, in_group(g))))

    await_sent(z, x)

    @pl.loop(jnp.maximum(me - 1, 1), me + 1)
    def _(t):
        await_sent(*place(t))

    for copy in weight_copies:
        copy.wait()

    exchange.wait_send()


CHUNKS = 8


def finish_kernel(heads, acc, qf_ref, kf_ref, hm_ref, w_ref, kw_ref, a_hbm, top_ref, w_hbm, kw_hbm, wb, kwb, ab, sem):
    for at, src, factor, buf, dst in ((0, w_ref, qf_ref, wb, w_hbm), (1, kw_ref, kf_ref, kwb, kw_hbm)):
        size = src.shape[0] // CHUNKS
        for i in range(CHUNKS):
            rows = pl.ds(i * size, size)
            buf[rows, :] = (src[rows, :].astype(jnp.float32) * factor[...]).astype(jnp.bfloat16)
            pltpu.make_async_copy(buf.at[rows], dst.at[rows], sem.at[at]).start()
    top_ref[...] = hm_ref[0, :heads]
    for h in range(heads):
        cols = slice(h * HEAD_SIZE, (h + 1) * HEAD_SIZE)
        a = acc[h]
        ab[:, cols] = (a[:HEAD_SIZE] / a[HEAD_SIZE:HEAD_SIZE + 1]).astype(jnp.bfloat16).T
        pltpu.make_async_copy(ab.at[:, cols], a_hbm.at[:, cols], sem.at[2]).start()
    for at, buf, dst in ((0, wb, w_hbm), (1, kwb, kw_hbm), (2, ab, a_hbm)):
        pltpu.make_async_copy(buf, dst, sem.at[at]).wait()


def shards(n, tp_n, queries, keys, values, w_query, key_weight):
    rows = queries.shape[0]
    heads = queries.shape[1] // HEAD_SIZE
    kv_heads = keys.shape[1] // HEAD_SIZE
    slots = n - 1 if n - 1 <= WINDOW else 1
    everyone = n * tp_n
    vmem = pl.BlockSpec(memory_space=pltpu.VMEM)
    hbm = pl.BlockSpec(memory_space=pltpu.HBM)
    dma = pltpu.SemaphoreType.DMA
    acc, q_factor, k_factor, maxima, w_local, kw_local = pl.pallas_call(
        functools.partial(attend_kernel, n, tp_n, heads, kv_heads, rows, slots),
        name="attend",
        out_shape=(
            jax.ShapeDtypeStruct((heads, HEAD_SIZE + SUMS, rows), jnp.float32),
            jax.ShapeDtypeStruct((1, heads * HEAD_SIZE), jnp.float32),
            jax.ShapeDtypeStruct((1, key_weight.shape[1]), jnp.float32),
            jax.ShapeDtypeStruct((1, LANES), jnp.float32),
            jax.ShapeDtypeStruct(w_query.shape, jnp.bfloat16),
            jax.ShapeDtypeStruct(key_weight.shape, jnp.bfloat16),
        ),
        in_specs=[hbm] * 5,
        out_specs=[vmem] * 6,
        scratch_shapes=[
            pltpu.VMEM((rows, heads * HEAD_SIZE), jnp.bfloat16),
            pltpu.VMEM((n, 2, kv_heads, rows, HEAD_SIZE), jnp.bfloat16),
            pltpu.VMEM((heads, HEAD_SIZE, rows), jnp.bfloat16),
            pltpu.VMEM((kv_heads, HEAD_SIZE + SUMS, rows), jnp.bfloat16),
            pltpu.VMEM((heads, 1, rows), jnp.float32),
            pltpu.VMEM((slots, heads, rows, rows), jnp.bfloat16),
            pltpu.VMEM((slots, heads, 1, rows), jnp.float32),
            pltpu.VMEM((1, LANES), jnp.float32),
            pltpu.VMEM((everyone, 1, LANES), jnp.float32),
            dma,
            dma,
            dma((2,)),
            dma((2, n, kv_heads)),
            dma((3, n)),
            dma,
            dma,
        ],
        compiler_params=pltpu.CompilerParams(
            collective_id=0, has_side_effects=True, vmem_limit_bytes=30 * 1024 * 1024
        ),
        cost_estimate=pl.CostEstimate(
            flops=4 * rows * rows * n * heads * HEAD_SIZE,
            bytes_accessed=4 * rows * heads * HEAD_SIZE,
            transcendentals=rows * rows * n * heads,
        ),
    )(*(
        pltpu.with_memory_space_constraint(a, pltpu.HBM)
        for a in (queries, keys, values, w_query, key_weight)
    ))
    return pl.pallas_call(
        functools.partial(finish_kernel, heads),
        name="finish",
        out_shape=(
            jax.ShapeDtypeStruct(queries.shape, jnp.bfloat16),
            jax.ShapeDtypeStruct((heads,), jnp.float32),
            jax.ShapeDtypeStruct(w_query.shape, jnp.bfloat16),
            jax.ShapeDtypeStruct(key_weight.shape, jnp.bfloat16),
        ),
        in_specs=[vmem] * 6,
        out_specs=(hbm, vmem, hbm, hbm),
        scratch_shapes=[
            pltpu.VMEM(w_query.shape, jnp.bfloat16),
            pltpu.VMEM(key_weight.shape, jnp.bfloat16),
            pltpu.VMEM(queries.shape, jnp.bfloat16),
            dma((3,)),
        ],
        compiler_params=pltpu.CompilerParams(vmem_limit_bytes=24 * 1024 * 1024),
        cost_estimate=pl.CostEstimate(
            flops=w_query.size + key_weight.size,
            bytes_accessed=4 * (w_query.size + key_weight.size),
            transcendentals=0,
        ),
    )(acc, q_factor, k_factor, maxima, w_local, kw_local)


def solution(mesh):
    in_specs = (P("seq", "tp"), P("seq", "tp"), P("seq", "tp"), P("seq", "tp"), P("seq", None))
    out_specs = (P("seq", "tp"), P("tp"), P("seq", "tp"), P("seq", None))
    body = functools.partial(shards, mesh.shape["seq"], mesh.shape["tp"])
    return jax.shard_map(body, mesh=mesh, in_specs=in_specs, out_specs=out_specs, check_vma=False)
```

```python
import functools
import math

import jax
import jax.numpy as jnp
from jax import lax
from jax.experimental import pallas as pl
from jax.experimental.pallas import tpu as pltpu
from jax.sharding import PartitionSpec as P

HEAD_SIZE = 128
LANES = 128
SUMS = 16
PARTS = 2

clip_threshold = 10.0
WINDOW = 7
UP, RIGHT, LEFT = range(3)
MESH = pl.DeviceIdType.MESH


def grid_of(n):
    columns = max(d for d in range(1, n + 1) if n % d == 0 and d * d <= n)
    return n // columns, columns


def attend_kernel(
    n, tp_n, heads, kv_heads, rows, slots,
    q_hbm, k_hbm, v_hbm, w_hbm, kw_hbm,
    acc, qf_ref, kf_ref, hm_ref, w_ref, kw_ref,
    qv, kv, qt, vt, mrun, pb, kp, mxl, mxb,
    lq, lkv, lw, recv, send, mx_recv, mx_send,
):
    group = heads // kv_heads
    nz, nx = grid_of(n)
    me = lax.axis_index("seq")
    tp = lax.axis_index("tp")
    z, x = lax.div(me, nx), lax.rem(me, nx)
    everyone = n * tp_n
    mine = me * tp_n + tp
    alone = slots == n - 1

    def head_cols(h):
        return pl.ds(h * HEAD_SIZE, HEAD_SIZE)

    def peer(d):
        other = lax.rem(mine + d, everyone)
        return {"seq": lax.div(other, tp_n), "tp": lax.rem(other, tp_n)}

    for g in range(kv_heads):
        for kind, hbm in enumerate((k_hbm, v_hbm)):
            pltpu.make_async_copy(hbm.at[:, head_cols(g)], kv.at[me, kind, g], lkv).start()
    q_copy = pltpu.make_async_copy(q_hbm, qv, lq)
    q_copy.start()

    barrier = pltpu.get_barrier_semaphore()

    @pl.loop(1, everyone)
    def _(d):
        pl.semaphore_signal(barrier, inc=1, device_id=peer(d), device_id_type=MESH)

    pltpu.make_async_copy(kv.at[me], kv.at[me], lkv).wait()
    pl.semaphore_wait(barrier, everyone - 1)

    part_rows = rows // PARTS

    def piece(kind, block, g, part, way, target):
        ref = kv.at[block, kind, g, pl.ds(part * part_rows, part_rows)]
        return pltpu.make_async_remote_copy(
            src_ref=ref, dst_ref=ref, send_sem=send.at[way, block],
            recv_sem=recv.at[kind, block, g, part],
            device_id={"seq": target}, device_id_type=MESH,
        )

    def routes(kind, row, col):
        up = col == x
        right = col <= x
        if kind == 1:
            up = up | ((row == z) & (col == x - 1))
            right = right & jnp.logical_not((row == z - 1) & (col == x))
        return (
            up & (z + 1 < nz),
            right & (x + 1 < nx),
            (col >= x) & (x > 0) & (row < z),
        )

    towards = (lax.rem(me + nx, n), lax.rem(me + 1, n), lax.rem(me + n - 1, n))

    def each_send(kind, g, row, col, ways=(UP, RIGHT, LEFT), parts=range(PARTS)):
        on = routes(kind, row, col)
        for way in ways:
            @pl.when(on[way])
            def _():
                for part in parts:
                    piece(kind, row * nx + col, g, part, way, towards[way]).start()

    def await_sent(row, col):
        block = row * nx + col
        for way, (key, value) in enumerate(zip(routes(0, row, col), routes(1, row, col))):
            def done(ref):
                pltpu.make_async_remote_copy(
                    src_ref=ref, dst_ref=ref, send_sem=send.at[way, block], recv_sem=recv.at[0, block, 0, 0],
                    device_id={"seq": towards[way]}, device_id_type=MESH,
                ).wait_send()

            @pl.when(key & value)
            def _():
                done(kv.at[block])

            @pl.when(key & jnp.logical_not(value))
            def _():
                done(kv.at[block, 0])

            @pl.when(value & jnp.logical_not(key))
            def _():
                done(kv.at[block, 1])

    for g in range(kv_heads):
        each_send(0, g, z, x, (UP, RIGHT))
    each_send(1, 0, z, x, (UP, RIGHT))

    def rest_of_own():
        for g in range(1, kv_heads):
            each_send(1, g, z, x, (UP, RIGHT))

    @pl.when(z == 0)
    def _():
        rest_of_own()

    q_copy.wait()

    scale = HEAD_SIZE ** (-0.5)
    to_exp2 = scale * math.log2(math.e)

    def place(t):
        below = jnp.where(z > 0, 1, 0)
        along = t - below
        beside = (along >= 1) & (along <= x)
        u = jnp.where(t == below, 0, jnp.maximum(t - x - 1, 0))
        w = jnp.maximum(u - 1, 0)
        k = 1 + lax.div(w, nx)
        j = lax.rem(w, nx) + jnp.where(k == z, 1, 0)
        up = jnp.where(u == 0, 1, jnp.where(j == 0, k + 1, k))
        left = jnp.where(u == 0, 0, j)
        row = jnp.where(beside, z, z - up)
        col = jnp.where(beside, x - along, lax.rem(x + nx - left, nx))
        return row, col

    def take(kind, g, t):
        row, col = place(t)
        for part in range(PARTS):
            piece(kind, row * nx + col, g, part, RIGHT, towards[RIGHT]).wait_recv()
            each_send(kind, g, row, col, parts=(part,))

    def own_part(g):
        vt[g, :HEAD_SIZE] = kv[me, 1, g].T
        r = lax.broadcasted_iota(jnp.int32, (rows, rows), 0)
        c = lax.broadcasted_iota(jnp.int32, (rows, rows), 1)
        for i in range(group):
            h = g * group + i
            s = lax.dot_general(
                kv[me, 0, g], qv[:, h * HEAD_SIZE:(h + 1) * HEAD_SIZE], (((1,), (1,)), ((), ())),
                preferred_element_type=jnp.float32,
            )
            s = jnp.where(c >= r, s, jnp.float32(-1e30))
            top = jnp.max(s, axis=0, keepdims=True)
            mrun[h] = top
            pb[0, h] = jnp.exp2((s - top) * to_exp2).astype(jnp.bfloat16)
        for i in range(group):
            h = g * group + i
            acc[h] = jnp.dot(vt[g], pb[0, h], preferred_element_type=jnp.float32)

    def score_part(g, t):
        row, col = place(t)
        block = row * nx + col
        slot = lax.rem(t - 1, slots)
        for i in range(group):
            h = g * group + i
            s = jnp.dot(kv[block, 0, g], qt[h], preferred_element_type=jnp.float32)
            old = mrun[h]
            top = jnp.maximum(old, jnp.max(s, axis=0, keepdims=True))
            mrun[h] = top
            kp[slot, h] = jnp.exp2((old - top) * to_exp2)
            pb[slot, h] = jnp.exp2((s - top) * to_exp2).astype(jnp.bfloat16)

    def value_part(g, t):
        row, col = place(t)
        slot = lax.rem(t - 1, slots)
        vt[g, :HEAD_SIZE] = kv[row * nx + col, 1, g].T
        for i in range(group):
            h = g * group + i
            acc[h] = acc[h] * kp[slot, h] + jnp.dot(
                vt[g], pb[slot, h], preferred_element_type=jnp.float32
            )

    for g in range(kv_heads):
        vt[g, HEAD_SIZE:] = jnp.ones((SUMS, rows), jnp.bfloat16)

    weight_copies = [
        pltpu.make_async_copy(w_hbm, w_ref, lw.at[0]), pltpu.make_async_copy(kw_hbm, kw_ref, lw.at[1])
    ]
    for copy in weight_copies:
        copy.start()

    for g in range(kv_heads):
        own_part(g)
    for h in range(heads):
        qt[h] = qv[:, h * HEAD_SIZE:(h + 1) * HEAD_SIZE].T

    def score_step(t):
        row, col = place(t)
        for g in range(kv_heads):
            take(0, g, t)
            if g == kv_heads - 1:
                @pl.when((row == 0) & (col == x))
                def _():
                    rest_of_own()
            score_part(g, t)

    last = z + 1 == nz

    def early(t):
        column = place(t)[1] == x
        return column & jnp.where(last, (x + 1 == nx) & (t == 1), z >= 1)

    def ahead(t):
        column = place(t)[1] == x
        return last & column & (t > 1) & (t <= me)

    def take_values(t):
        for g in range(kv_heads):
            take(1, g, t)

    def value_step(t):
        if alone:
            @pl.when(last & (t > 1) & jnp.logical_not(ahead(t)))
            def _():
                take_values(t)

            @pl.when((t > 1) & ahead(t + 2))
            def _():
                take_values(t + 2)
        else:
            take_values(t)

        for g in range(kv_heads):
            value_part(g, t)
        @pl.when(t > 2)
        def _():
            await_sent(*place(t - 2))

    lane = lax.broadcasted_iota(jnp.int32, (1, LANES), 1)
    def mx_copy(d, owner):
        return pltpu.make_async_remote_copy(
            src_ref=mxl, dst_ref=mxb.at[owner], send_sem=mx_send,
            recv_sem=mx_recv, device_id=peer(d), device_id_type=MESH,
        )

    def send_maxima():
        local = jnp.full((1, LANES), -1e30, jnp.float32)
        for h in range(heads):
            local = jnp.where(lane == h, jnp.max(mrun[h], axis=1, keepdims=True), local)
        mxl[...] = local
        mxb[mine] = local

        @pl.loop(1, everyone)
        def _(d):
            mx_copy(d, mine).start()

    if alone:
        @pl.loop(1, me + 1)
        def _(t):
            @pl.when(t == me)
            def _():
                @pl.loop(1, me + 1)
                def _(s):
                    @pl.when(early(s))
                    def _():
                        take_values(s)

            score_step(t)

        @pl.when(last & (me > 0))
        def _():
            @pl.when(jnp.logical_not(early(1)))
            def _():
                take_values(1)

            for t in (2, 3):
                @pl.when(ahead(t))
                def _():
                    take_values(t)

        send_maxima()

        @pl.loop(1, jnp.where(last, 1, me + 1))
        def _(t):
            @pl.when(jnp.logical_not(early(t)))
            def _():
                take_values(t)

        @pl.loop(1, me + 1)
        def _(t):
            value_step(t)
    else:
        @pl.loop(1, me + 1)
        def _(t):
            score_step(t)
            value_step(t)

        send_maxima()

    others = mxb.at[pl.ds(0, everyone - 1)]
    exchange = pltpu.make_async_remote_copy(
        src_ref=others, dst_ref=others, send_sem=mx_send, recv_sem=mx_recv,
        device_id=peer(1), device_id_type=MESH,
    )
    exchange.wait_recv()

    def widest_lanes(a, keep):
        return jnp.broadcast_to(
            jnp.max(jnp.where(keep, a, -1e30), axis=1, keepdims=True), (1, LANES)
        )

    def clip_of(top):
        return clip_threshold / jnp.maximum(top * scale, clip_threshold)

    def shard_top(owner):
        top = mxb[owner]
        for i in range(1, n):
            top = jnp.maximum(top, mxb[i * tp_n + owner])
        return top

    def in_group(g):
        return (lane >= g * group) & (lane < (g + 1) * group)

    top = shard_top(tp)
    hm_ref[...] = top * scale
    clip = [clip_of(widest_lanes(top, in_group(g))) for g in range(kv_heads)]
    for h in range(heads):
        qf_ref[:, h * HEAD_SIZE:(h + 1) * HEAD_SIZE] = clip_of(
            widest_lanes(top, lane == h)
        ) / jnp.sqrt(clip[h // group])
    for owner in range(tp_n):
        other = shard_top(owner)
        for g in range(kv_heads):
            at = (owner * kv_heads + g) * HEAD_SIZE
            kf_ref[:, at:at + HEAD_SIZE] = jnp.sqrt(clip_of(widest_lanes(other, in_group(g))))

    await_sent(z, x)

    @pl.loop(jnp.maximum(me - 1, 1), me + 1)
    def _(t):
        await_sent(*place(t))

    for copy in weight_copies:
        copy.wait()

    exchange.wait_send()


CHUNKS = 8


def finish_kernel(heads, acc, qf_ref, kf_ref, hm_ref, w_ref, kw_ref, a_hbm, top_ref, w_hbm, kw_hbm, wb, kwb, ab, sem):
    for at, src, factor, buf, dst in ((0, w_ref, qf_ref, wb, w_hbm), (1, kw_ref, kf_ref, kwb, kw_hbm)):
        size = src.shape[0] // CHUNKS
        for i in range(CHUNKS):
            rows = pl.ds(i * size, size)
            buf[rows, :] = (src[rows, :].astype(jnp.float32) * factor[...]).astype(jnp.bfloat16)
            pltpu.make_async_copy(buf.at[rows], dst.at[rows], sem.at[at]).start()
    top_ref[...] = hm_ref[0, :heads]
    for h in range(heads):
        cols = slice(h * HEAD_SIZE, (h + 1) * HEAD_SIZE)
        a = acc[h]
        ab[:, cols] = (a[:HEAD_SIZE] / a[HEAD_SIZE:HEAD_SIZE + 1]).astype(jnp.bfloat16).T
        pltpu.make_async_copy(ab.at[:, cols], a_hbm.at[:, cols], sem.at[2]).start()
    for at, buf, dst in ((0, wb, w_hbm), (1, kwb, kw_hbm), (2, ab, a_hbm)):
        pltpu.make_async_copy(buf, dst, sem.at[at]).wait()


def shards(n, tp_n, queries, keys, values, w_query, key_weight):
    rows = queries.shape[0]
    heads = queries.shape[1] // HEAD_SIZE
    kv_heads = keys.shape[1] // HEAD_SIZE
    slots = n - 1 if n - 1 <= WINDOW else 1
    everyone = n * tp_n
    vmem = pl.BlockSpec(memory_space=pltpu.VMEM)
    hbm = pl.BlockSpec(memory_space=pltpu.HBM)
    dma = pltpu.SemaphoreType.DMA
    acc, q_factor, k_factor, maxima, w_local, kw_local = pl.pallas_call(
        functools.partial(attend_kernel, n, tp_n, heads, kv_heads, rows, slots),
        name="attend",
        out_shape=(
            jax.ShapeDtypeStruct((heads, HEAD_SIZE + SUMS, rows), jnp.float32),
            jax.ShapeDtypeStruct((1, heads * HEAD_SIZE), jnp.float32),
            jax.ShapeDtypeStruct((1, key_weight.shape[1]), jnp.float32),
            jax.ShapeDtypeStruct((1, LANES), jnp.float32),
            jax.ShapeDtypeStruct(w_query.shape, jnp.bfloat16),
            jax.ShapeDtypeStruct(key_weight.shape, jnp.bfloat16),
        ),
        in_specs=[hbm] * 5,
        out_specs=[vmem] * 6,
        scratch_shapes=[
            pltpu.VMEM((rows, heads * HEAD_SIZE), jnp.bfloat16),
            pltpu.VMEM((n, 2, kv_heads, rows, HEAD_SIZE), jnp.bfloat16),
            pltpu.VMEM((heads, HEAD_SIZE, rows), jnp.bfloat16),
            pltpu.VMEM((kv_heads, HEAD_SIZE + SUMS, rows), jnp.bfloat16),
            pltpu.VMEM((heads, 1, rows), jnp.float32),
            pltpu.VMEM((slots, heads, rows, rows), jnp.bfloat16),
            pltpu.VMEM((slots, heads, 1, rows), jnp.float32),
            pltpu.VMEM((1, LANES), jnp.float32),
            pltpu.VMEM((everyone, 1, LANES), jnp.float32),
            dma,
            dma,
            dma((2,)),
            dma((2, n, kv_heads, PARTS)),
            dma((3, n)),
            dma,
            dma,
        ],
        compiler_params=pltpu.CompilerParams(
            collective_id=0, has_side_effects=True, vmem_limit_bytes=30 * 1024 * 1024
        ),
        cost_estimate=pl.CostEstimate(
            flops=4 * rows * rows * n * heads * HEAD_SIZE,
            bytes_accessed=4 * rows * heads * HEAD_SIZE,
            transcendentals=rows * rows * n * heads,
        ),
    )(*(
        pltpu.with_memory_space_constraint(a, pltpu.HBM)
        for a in (queries, keys, values, w_query, key_weight)
    ))
    return pl.pallas_call(
        functools.partial(finish_kernel, heads),
        name="finish",
        out_shape=(
            jax.ShapeDtypeStruct(queries.shape, jnp.bfloat16),
            jax.ShapeDtypeStruct((heads,), jnp.float32),
            jax.ShapeDtypeStruct(w_query.shape, jnp.bfloat16),
            jax.ShapeDtypeStruct(key_weight.shape, jnp.bfloat16),
        ),
        in_specs=[vmem] * 6,
        out_specs=(hbm, vmem, hbm, hbm),
        scratch_shapes=[
            pltpu.VMEM(w_query.shape, jnp.bfloat16),
            pltpu.VMEM(key_weight.shape, jnp.bfloat16),
            pltpu.VMEM(queries.shape, jnp.bfloat16),
            dma((3,)),
        ],
        compiler_params=pltpu.CompilerParams(vmem_limit_bytes=24 * 1024 * 1024),
        cost_estimate=pl.CostEstimate(
            flops=w_query.size + key_weight.size,
            bytes_accessed=4 * (w_query.size + key_weight.size),
            transcendentals=0,
        ),
    )(acc, q_factor, k_factor, maxima, w_local, kw_local)


def solution(mesh):
    in_specs = (P("seq", "tp"), P("seq", "tp"), P("seq", "tp"), P("seq", "tp"), P("seq", None))
    out_specs = (P("seq", "tp"), P("tp"), P("seq", "tp"), P("seq", None))
    body = functools.partial(shards, mesh.shape["seq"], mesh.shape["tp"])
    return jax.shard_map(body, mesh=mesh, in_specs=in_specs, out_specs=out_specs, check_vma=False)
```

```python
import functools
import math

import jax
import jax.numpy as jnp
from jax import lax
from jax.experimental import pallas as pl
from jax.experimental.pallas import tpu as pltpu
from jax.sharding import PartitionSpec as P

HEAD_SIZE = 128
LANES = 128
SUMS = 16
PARTS = 2

clip_threshold = 10.0
WINDOW = 7
UP, RIGHT, LEFT = range(3)
MESH = pl.DeviceIdType.MESH


def grid_of(n):
    columns = max(d for d in range(1, n + 1) if n % d == 0 and d * d <= n)
    return n // columns, columns


def attend_kernel(
    n, tp_n, heads, kv_heads, rows, slots,
    q_hbm, k_hbm, v_hbm, w_hbm, kw_hbm,
    acc, qf_ref, kf_ref, hm_ref, w_ref, kw_ref,
    qv, kv, qt, vt, mrun, pb, kp, mxl, mxb,
    lq, lkv, lw, recv, send, mx_recv, mx_send,
):
    group = heads // kv_heads
    nz, nx = grid_of(n)
    me = lax.axis_index("seq")
    tp = lax.axis_index("tp")
    z, x = lax.div(me, nx), lax.rem(me, nx)
    everyone = n * tp_n
    mine = me * tp_n + tp
    alone = slots == n - 1

    def head_cols(h):
        return pl.ds(h * HEAD_SIZE, HEAD_SIZE)

    columns = [lax.rem(tp + e, tp_n) for e in range(tp_n)]

    def each_peer(act):
        @pl.loop(0, n)
        def _(d):
            row = lax.rem(me + d, n)

            @pl.when(d > 0)
            def _():
                act({"seq": row, "tp": tp})

            for e in range(1, tp_n):
                act({"seq": row, "tp": columns[e]})

    for g in range(kv_heads):
        for kind, hbm in enumerate((k_hbm, v_hbm)):
            pltpu.make_async_copy(hbm.at[:, head_cols(g)], kv.at[me, kind, g], lkv).start()
    q_copy = pltpu.make_async_copy(q_hbm, qv, lq)
    q_copy.start()

    barrier = pltpu.get_barrier_semaphore()

    each_peer(lambda peer: pl.semaphore_signal(barrier, inc=1, device_id=peer, device_id_type=MESH))

    pltpu.make_async_copy(kv.at[me], kv.at[me], lkv).wait()
    pl.semaphore_wait(barrier, everyone - 1)

    part_rows = rows // PARTS

    def piece(kind, block, g, part, way, target):
        ref = kv.at[block, kind, g, pl.ds(part * part_rows, part_rows)]
        return pltpu.make_async_remote_copy(
            src_ref=ref, dst_ref=ref, send_sem=send.at[way, block],
            recv_sem=recv.at[kind, block, g, part],
            device_id={"seq": target}, device_id_type=MESH,
        )

    def routes(kind, row, col):
        up = col == x
        right = col <= x
        if kind == 1:
            up = up | ((row == z) & (col == x - 1))
            right = right & jnp.logical_not((row == z - 1) & (col == x))
        return (
            up & (z + 1 < nz),
            right & (x + 1 < nx),
            (col >= x) & (x > 0) & (row < z),
        )

    towards = (lax.rem(me + nx, n), lax.rem(me + 1, n), lax.rem(me + n - 1, n))

    def each_send(kind, g, row, col, ways=(UP, RIGHT, LEFT), parts=range(PARTS)):
        on = routes(kind, row, col)
        for way in ways:
            @pl.when(on[way])
            def _():
                for part in parts:
                    piece(kind, row * nx + col, g, part, way, towards[way]).start()

    def await_sent(row, col):
        block = row * nx + col
        for way, (key, value) in enumerate(zip(routes(0, row, col), routes(1, row, col))):
            def done(ref):
                pltpu.make_async_remote_copy(
                    src_ref=ref, dst_ref=ref, send_sem=send.at[way, block], recv_sem=recv.at[0, block, 0, 0],
                    device_id={"seq": towards[way]}, device_id_type=MESH,
                ).wait_send()

            @pl.when(key & value)
            def _():
                done(kv.at[block])

            @pl.when(key & jnp.logical_not(value))
            def _():
                done(kv.at[block, 0])

            @pl.when(value & jnp.logical_not(key))
            def _():
                done(kv.at[block, 1])

    for g in range(kv_heads):
        each_send(0, g, z, x, (UP, RIGHT))
    each_send(1, 0, z, x, (UP, RIGHT))

    def rest_of_own():
        for g in range(1, kv_heads):
            each_send(1, g, z, x, (UP, RIGHT))

    @pl.when(z == 0)
    def _():
        rest_of_own()

    q_copy.wait()

    scale = HEAD_SIZE ** (-0.5)
    to_exp2 = scale * math.log2(math.e)

    def place(t):
        below = jnp.where(z > 0, 1, 0)
        along = t - below
        beside = (along >= 1) & (along <= x)
        u = jnp.where(t == below, 0, jnp.maximum(t - x - 1, 0))
        w = jnp.maximum(u - 1, 0)
        k = 1 + lax.div(w, nx)
        j = lax.rem(w, nx) + jnp.where(k == z, 1, 0)
        up = jnp.where(u == 0, 1, jnp.where(j == 0, k + 1, k))
        left = jnp.where(u == 0, 0, j)
        row = jnp.where(beside, z, z - up)
        col = jnp.where(beside, x - along, lax.rem(x + nx - left, nx))
        return row, col

    def take(kind, g, t):
        row, col = place(t)
        for part in range(PARTS):
            piece(kind, row * nx + col, g, part, RIGHT, towards[RIGHT]).wait_recv()
            each_send(kind, g, row, col, parts=(part,))

    def own_part(g):
        vt[g, :HEAD_SIZE] = kv[me, 1, g].T
        r = lax.broadcasted_iota(jnp.int32, (rows, rows), 0)
        c = lax.broadcasted_iota(jnp.int32, (rows, rows), 1)
        for i in range(group):
            h = g * group + i
            s = lax.dot_general(
                kv[me, 0, g], qv[:, h * HEAD_SIZE:(h + 1) * HEAD_SIZE], (((1,), (1,)), ((), ())),
                preferred_element_type=jnp.float32,
            )
            s = jnp.where(c >= r, s, jnp.float32(-1e30))
            top = jnp.max(s, axis=0, keepdims=True)
            mrun[h] = top
            pb[0, h] = jnp.exp2((s - top) * to_exp2).astype(jnp.bfloat16)
        for i in range(group):
            h = g * group + i
            acc[h] = jnp.dot(vt[g], pb[0, h], preferred_element_type=jnp.float32)

    def score_part(g, t):
        row, col = place(t)
        block = row * nx + col
        slot = lax.rem(t - 1, slots)
        for i in range(group):
            h = g * group + i
            s = jnp.dot(kv[block, 0, g], qt[h], preferred_element_type=jnp.float32)
            old = mrun[h]
            top = jnp.maximum(old, jnp.max(s, axis=0, keepdims=True))
            mrun[h] = top
            kp[slot, h] = jnp.exp2((old - top) * to_exp2)
            pb[slot, h] = jnp.exp2((s - top) * to_exp2).astype(jnp.bfloat16)

    def value_part(g, t):
        row, col = place(t)
        slot = lax.rem(t - 1, slots)
        vt[g, :HEAD_SIZE] = kv[row * nx + col, 1, g].T
        for i in range(group):
            h = g * group + i
            acc[h] = acc[h] * kp[slot, h] + jnp.dot(
                vt[g], pb[slot, h], preferred_element_type=jnp.float32
            )

    for g in range(kv_heads):
        vt[g, HEAD_SIZE:] = jnp.ones((SUMS, rows), jnp.bfloat16)

    weight_copies = [
        pltpu.make_async_copy(w_hbm, w_ref, lw.at[0]), pltpu.make_async_copy(kw_hbm, kw_ref, lw.at[1])
    ]
    for copy in weight_copies:
        copy.start()

    for g in range(kv_heads):
        own_part(g)
    for h in range(heads):
        qt[h] = qv[:, h * HEAD_SIZE:(h + 1) * HEAD_SIZE].T

    def score_step(t):
        row, col = place(t)
        for g in range(kv_heads):
            take(0, g, t)
            if g == kv_heads - 1:
                @pl.when((row == 0) & (col == x))
                def _():
                    rest_of_own()
            score_part(g, t)

    last = z + 1 == nz

    def early(t):
        column = place(t)[1] == x
        return column & jnp.where(last, (x + 1 == nx) & (t == 1), z >= 1)

    def ahead(t):
        column = place(t)[1] == x
        return last & column & (t > 1) & (t <= me)

    def take_values(t):
        for g in range(kv_heads):
            take(1, g, t)

    def value_step(t):
        if alone:
            @pl.when(last & (t > 1) & jnp.logical_not(ahead(t)))
            def _():
                take_values(t)

            @pl.when((t > 1) & ahead(t + 2))
            def _():
                take_values(t + 2)
        else:
            take_values(t)

        for g in range(kv_heads):
            value_part(g, t)
        @pl.when(t > 2)
        def _():
            await_sent(*place(t - 2))

    lane = lax.broadcasted_iota(jnp.int32, (1, LANES), 1)
    def mx_copy(peer):
        return pltpu.make_async_remote_copy(
            src_ref=mxl, dst_ref=mxb.at[mine], send_sem=mx_send,
            recv_sem=mx_recv, device_id=peer, device_id_type=MESH,
        )

    def send_maxima():
        local = jnp.full((1, LANES), -1e30, jnp.float32)
        for h in range(heads):
            local = jnp.where(lane == h, jnp.max(mrun[h], axis=1, keepdims=True), local)
        mxl[...] = local
        mxb[mine] = local

        each_peer(lambda peer: mx_copy(peer).start())

    if alone:
        @pl.loop(1, me + 1)
        def _(t):
            @pl.when(t == me)
            def _():
                @pl.loop(1, me + 1)
                def _(s):
                    @pl.when(early(s))
                    def _():
                        take_values(s)

            score_step(t)

        @pl.when(last & (me > 0))
        def _():
            @pl.when(jnp.logical_not(early(1)))
            def _():
                take_values(1)

            for t in (2, 3):
                @pl.when(ahead(t))
                def _():
                    take_values(t)

        send_maxima()

        @pl.loop(1, jnp.where(last, 1, me + 1))
        def _(t):
            @pl.when(jnp.logical_not(early(t)))
            def _():
                take_values(t)

        @pl.loop(1, me + 1)
        def _(t):
            value_step(t)
    else:
        @pl.loop(1, me + 1)
        def _(t):
            score_step(t)
            value_step(t)

        send_maxima()

    others = mxb.at[pl.ds(0, everyone - 1)]
    exchange = pltpu.make_async_remote_copy(
        src_ref=others, dst_ref=others, send_sem=mx_send, recv_sem=mx_recv,
        device_id={"seq": towards[RIGHT]}, device_id_type=MESH,
    )
    exchange.wait_recv()

    def widest_lanes(a, keep):
        return jnp.broadcast_to(
            jnp.max(jnp.where(keep, a, -1e30), axis=1, keepdims=True), (1, LANES)
        )

    def clip_of(top):
        return clip_threshold / jnp.maximum(top * scale, clip_threshold)

    def shard_top(owner):
        top = mxb[owner]
        for i in range(1, n):
            top = jnp.maximum(top, mxb[i * tp_n + owner])
        return top

    def in_group(g):
        return (lane >= g * group) & (lane < (g + 1) * group)

    top = shard_top(tp)
    hm_ref[...] = top * scale
    clip = [clip_of(widest_lanes(top, in_group(g))) for g in range(kv_heads)]
    for h in range(heads):
        qf_ref[:, h * HEAD_SIZE:(h + 1) * HEAD_SIZE] = clip_of(
            widest_lanes(top, lane == h)
        ) / jnp.sqrt(clip[h // group])
    for owner in range(tp_n):
        other = shard_top(owner)
        for g in range(kv_heads):
            at = (owner * kv_heads + g) * HEAD_SIZE
            kf_ref[:, at:at + HEAD_SIZE] = jnp.sqrt(clip_of(widest_lanes(other, in_group(g))))

    await_sent(z, x)

    @pl.loop(jnp.maximum(me - 1, 1), me + 1)
    def _(t):
        await_sent(*place(t))

    for copy in weight_copies:
        copy.wait()

    exchange.wait_send()


CHUNKS = 8


def finish_kernel(heads, acc, qf_ref, kf_ref, hm_ref, w_ref, kw_ref, a_hbm, top_ref, w_hbm, kw_hbm, wb, kwb, ab, sem):
    for at, src, factor, buf, dst in ((0, w_ref, qf_ref, wb, w_hbm), (1, kw_ref, kf_ref, kwb, kw_hbm)):
        size = src.shape[0] // CHUNKS
        for i in range(CHUNKS):
            rows = pl.ds(i * size, size)
            buf[rows, :] = (src[rows, :].astype(jnp.float32) * factor[...]).astype(jnp.bfloat16)
            pltpu.make_async_copy(buf.at[rows], dst.at[rows], sem.at[at]).start()
    top_ref[...] = hm_ref[0, :heads]
    for h in range(heads):
        cols = slice(h * HEAD_SIZE, (h + 1) * HEAD_SIZE)
        a = acc[h]
        ab[:, cols] = (a[:HEAD_SIZE] / a[HEAD_SIZE:HEAD_SIZE + 1]).astype(jnp.bfloat16).T
        pltpu.make_async_copy(ab.at[:, cols], a_hbm.at[:, cols], sem.at[2]).start()
    for at, buf, dst in ((0, wb, w_hbm), (1, kwb, kw_hbm), (2, ab, a_hbm)):
        pltpu.make_async_copy(buf, dst, sem.at[at]).wait()


def shards(n, tp_n, queries, keys, values, w_query, key_weight):
    rows = queries.shape[0]
    heads = queries.shape[1] // HEAD_SIZE
    kv_heads = keys.shape[1] // HEAD_SIZE
    slots = n - 1 if n - 1 <= WINDOW else 1
    everyone = n * tp_n
    vmem = pl.BlockSpec(memory_space=pltpu.VMEM)
    hbm = pl.BlockSpec(memory_space=pltpu.HBM)
    dma = pltpu.SemaphoreType.DMA
    acc, q_factor, k_factor, maxima, w_local, kw_local = pl.pallas_call(
        functools.partial(attend_kernel, n, tp_n, heads, kv_heads, rows, slots),
        name="attend",
        out_shape=(
            jax.ShapeDtypeStruct((heads, HEAD_SIZE + SUMS, rows), jnp.float32),
            jax.ShapeDtypeStruct((1, heads * HEAD_SIZE), jnp.float32),
            jax.ShapeDtypeStruct((1, key_weight.shape[1]), jnp.float32),
            jax.ShapeDtypeStruct((1, LANES), jnp.float32),
            jax.ShapeDtypeStruct(w_query.shape, jnp.bfloat16),
            jax.ShapeDtypeStruct(key_weight.shape, jnp.bfloat16),
        ),
        in_specs=[hbm] * 5,
        out_specs=[vmem] * 6,
        scratch_shapes=[
            pltpu.VMEM((rows, heads * HEAD_SIZE), jnp.bfloat16),
            pltpu.VMEM((n, 2, kv_heads, rows, HEAD_SIZE), jnp.bfloat16),
            pltpu.VMEM((heads, HEAD_SIZE, rows), jnp.bfloat16),
            pltpu.VMEM((kv_heads, HEAD_SIZE + SUMS, rows), jnp.bfloat16),
            pltpu.VMEM((heads, 1, rows), jnp.float32),
            pltpu.VMEM((slots, heads, rows, rows), jnp.bfloat16),
            pltpu.VMEM((slots, heads, 1, rows), jnp.float32),
            pltpu.VMEM((1, LANES), jnp.float32),
            pltpu.VMEM((everyone, 1, LANES), jnp.float32),
            dma,
            dma,
            dma((2,)),
            dma((2, n - 1, kv_heads, PARTS)),
            dma((3, n - 1)),
            dma,
            dma,
        ],
        compiler_params=pltpu.CompilerParams(
            collective_id=0, has_side_effects=True, vmem_limit_bytes=30 * 1024 * 1024
        ),
        cost_estimate=pl.CostEstimate(
            flops=4 * rows * rows * n * heads * HEAD_SIZE,
            bytes_accessed=4 * rows * heads * HEAD_SIZE,
            transcendentals=rows * rows * n * heads,
        ),
    )(*(
        pltpu.with_memory_space_constraint(a, pltpu.HBM)
        for a in (queries, keys, values, w_query, key_weight)
    ))
    return pl.pallas_call(
        functools.partial(finish_kernel, heads),
        name="finish",
        out_shape=(
            jax.ShapeDtypeStruct(queries.shape, jnp.bfloat16),
            jax.ShapeDtypeStruct((heads,), jnp.float32),
            jax.ShapeDtypeStruct(w_query.shape, jnp.bfloat16),
            jax.ShapeDtypeStruct(key_weight.shape, jnp.bfloat16),
        ),
        in_specs=[vmem] * 6,
        out_specs=(hbm, vmem, hbm, hbm),
        scratch_shapes=[
            pltpu.VMEM(w_query.shape, jnp.bfloat16),
            pltpu.VMEM(key_weight.shape, jnp.bfloat16),
            pltpu.VMEM(queries.shape, jnp.bfloat16),
            dma((3,)),
        ],
        compiler_params=pltpu.CompilerParams(vmem_limit_bytes=24 * 1024 * 1024),
        cost_estimate=pl.CostEstimate(
            flops=w_query.size + key_weight.size,
            bytes_accessed=4 * (w_query.size + key_weight.size),
            transcendentals=0,
        ),
    )(acc, q_factor, k_factor, maxima, w_local, kw_local)


def solution(mesh):
    in_specs = (P("seq", "tp"), P("seq", "tp"), P("seq", "tp"), P("seq", "tp"), P("seq", None))
    out_specs = (P("seq", "tp"), P("tp"), P("seq", "tp"), P("seq", None))
    body = functools.partial(shards, mesh.shape["seq"], mesh.shape["tp"])
    return jax.shard_map(body, mesh=mesh, in_specs=in_specs, out_specs=out_specs, check_vma=False)
```
